32 devices in a mesh: layer: 4 (over y, core), col: 4 (over z), row: 2 (over x).
Axes of the slice: x: 2, y: 2, z: 4, core: 2. Of those that a mesh axis runs over, the one named last changes fastest.
Arguments:
- activations: bfloat16 [4, 768, 4096], P(None, ('layer', 'row'), 'col'), may hold values from -6 to 6
- out_grads: bfloat16 [4, 768, 11008], P(None, ('layer', 'col'), 'row'), may hold values from -0.02734375 to 0.02734375
- basis_in: bfloat16 [4, 4096, 4096], P('layer', 'col', 'row'), may hold values from -0.09375 to 0.09375
- basis_out: bfloat16 [4, 11008, 11008], P('layer', 'row', 'col'), may hold values from -0.0546875 to 0.0546875
- eigenvalues: float32 [4, 11008, 4096], P('layer', 'col', 'row'), may hold values from 0.01 to 10
- damping: float32 [4], P('layer'), may hold values from 0.05 to 0.5
- layer_order: int32 [4], replicated, may hold values from 0 to 3, each once
- query_ids: int32 [256], replicated, may hold values from 0 to 3, never falling along the last dimension, each value on 1 to 128 neighbouring positions
- train_ids: int32 [512], replicated, may hold values from 0 to 15, never falling along the last dimension, each value on 1 to 64 neighbouring positions
Outputs:
- scores: float32 [4, 16], replicated
The draws below stay inside these ranges and needn't reach their ends.
Inputs may be any that keep to these rules, and one draw needn't show every extreme that they name: `layer_order`: each slot's layer appears once. `query_ids`: never falling; every query example has 1 to 128 tokens. `train_ids`: never falling; every train example has 1 to 64 tokens.
All inputs are finite; a program needn't handle non-finite values.
Results may differ from the reference program's by a relative error of at most 0.02.
Values may be sent and summed in bfloat16 or wider, within the bound.
A program may use at most 192 MiB of HBM per device.

```python
import math
import jax
import jax.numpy as jnp
import numpy as np
from jax import lax

DIN = 4096
DOUT = 11008
LAYERS = 4
QUERIES = 4
TRAIN = 16
QLEN = 64
TLEN = 32
QTOK = 256
TTOK = 512
QMOST = 128
TMOST = 64
N_COL = 4
N_ROW = 2


def level_of(stream_key, shape, cuts, least, top_value):
    gain = 1.0
    for position, parts in cuts:
        draws = jax.random.uniform(jax.random.fold_in(jax.random.fold_in(stream_key, 6), position), (parts,), jnp.float32, least / len(cuts), top_value / len(cuts))
        gain = gain * jnp.repeat(jnp.exp(draws), shape[position] // parts).reshape((-1,) + (1,) * (len(shape) - 1 - position))
    return gain


def length_profile(number_of, total, bound, lean):
    weights = [(1 << 20) // math.isqrt(standing ** lean) + 1 for standing in range(2, number_of + 1)]
    rest, holding = total - bound - (number_of - 1), [1] * (number_of - 1)
    while rest > 0:
        free = [i for i in range(number_of - 1) if holding[i] < bound]
        mass, remaining = sum([weights[i] for i in free]), rest
        for i in free:
            addition = min(bound - holding[i], max(1, remaining * weights[i] // mass), rest)
            holding[i] = holding[i] + addition
            rest = rest - addition
    return np.array([bound] + holding)


def ragged_sizes(rng, amount, total, most, skew):
    if amount == 2:
        one = jax.random.randint(rng, (), max(1, total - most), min(most, total - 1) + 1)
        return jnp.stack([one, total - one])
    lengths = jnp.asarray(length_profile(amount, total, most, skew), jnp.int32)
    twos = (amount - 1) // 2
    giver, receiver = lengths[1:1 + 2 * twos:2], lengths[2:2 + 2 * twos:2]
    room = jnp.minimum(giver - 1, most - receiver)
    moved = jax.random.randint(jax.random.fold_in(rng, 1), (twos,), 0, 1 << 20) % (room + 1)
    lengths = lengths.at[1:1 + 2 * twos:2].set(giver - moved).at[2:2 + 2 * twos:2].set(receiver + moved)
    return lengths[jax.random.permutation(jax.random.fold_in(rng, 2), amount)]


def normal_values(stream_key, extent, spread, reach, pieces=(), kind=jnp.bfloat16):
    array = spread * jax.random.normal(stream_key, extent, jnp.float32)
    if pieces:
        array = array * level_of(stream_key, extent, pieces, -0.22, 0.18)
    return jnp.clip(array, -reach, reach).astype(kind)


def setup_inputs(seed: int = 0) -> dict:
    streams_of = jax.random.split(jax.random.key(seed), 10)
    activations = normal_values(streams_of[0], (LAYERS, QTOK + TTOK, DIN), 1.0, 6.0, ((1, 8), (2, 4)))
    out_grads = normal_values(streams_of[1], (LAYERS, QTOK + TTOK, DOUT), ((QLEN * TLEN * DIN * DOUT) ** -0.25), 0.02734375, ((1, 16), (2, 2)))
    basis_in = normal_values(streams_of[2], (LAYERS, DIN, DIN), DIN ** -0.5, 0.09375, ((0, 4), (1, 4), (2, 2)))
    basis_out = normal_values(streams_of[3], (LAYERS, DOUT, DOUT), DOUT ** -0.5, 0.0546875, ((0, 4), (1, 2), (2, 4)))
    eigenvalues = jnp.clip(jnp.exp(math.log(10.0) - 6.9077553 * jax.random.uniform(streams_of[4], (LAYERS, DOUT, DIN), jnp.float32) ** level_of(streams_of[4], (LAYERS, DOUT, DIN), ((0, 4), (1, 4), (2, 2)), -0.2, 0.2)), 0.01, 10.0)
    damping = jnp.clip(jnp.exp(math.log(0.5) - 2.3025851 * jax.random.uniform(streams_of[5], (LAYERS,), jnp.float32) ** level_of(streams_of[5], (LAYERS,), ((0, 4),), -0.2, 0.2)), 0.05, 0.5)
    layer_order = jax.random.permutation(streams_of[6], LAYERS).astype(jnp.int32)
    query_ids = jnp.searchsorted(jnp.cumsum(ragged_sizes(streams_of[7], QUERIES, QTOK, QMOST, 1)), jnp.arange(QTOK), side="right").astype(jnp.int32)
    train_ids = jnp.searchsorted(jnp.cumsum(ragged_sizes(streams_of[8], TRAIN, TTOK, TMOST, 1)), jnp.arange(TTOK), side="right").astype(jnp.int32)
    return {"activations": activations, "out_grads": out_grads, "basis_in": basis_in, "basis_out": basis_out, "eigenvalues": eigenvalues, "damping": damping, "layer_order": layer_order, "query_ids": query_ids, "train_ids": train_ids}


def rotate(values, basis, blocks):
    width = basis.shape[0] // blocks
    total = jnp.zeros((values.shape[0], basis.shape[1]), jnp.float32)
    for index in range(blocks):
        piece = jnp.dot(values[:, index * width:(index + 1) * width], basis[index * width:(index + 1) * width], preferred_element_type=jnp.float32)
        rounded = lax.optimization_barrier(piece.astype(jnp.bfloat16))
        total = total + rounded.astype(jnp.float32)
    return total.astype(jnp.bfloat16)


def reference(activations, out_grads, basis_in, basis_out, eigenvalues, damping, layer_order, query_ids, train_ids):
    query_tokens = query_ids.shape[0]
    train_onehot = (train_ids[:, None] == jnp.arange(TRAIN, dtype=jnp.int32)[None, :]).astype(jnp.float32)
    total = jnp.zeros((QUERIES, TRAIN), jnp.float32)
    for slot in range(LAYERS):
        layer = layer_order[slot].astype(jnp.int32)
        inputs = lax.dynamic_index_in_dim(activations, layer, 0, keepdims=False)
        grads = lax.dynamic_index_in_dim(out_grads, layer, 0, keepdims=False)
        rotated_in = rotate(inputs, basis_in[slot], N_COL)
        rotated_out = rotate(grads, basis_out[slot], N_ROW)
        query_in = rotated_in[:query_tokens]
        query_out = rotated_out[:query_tokens]
        train_in = rotated_in[query_tokens:]
        train_out = rotated_out[query_tokens:]
        denominator = eigenvalues[slot] + damping[slot]

        def one_query(index):
            mask = (query_ids == index).astype(jnp.bfloat16)
            masked = query_in * mask[:, None]
            gram = jnp.dot(query_out.T, masked, preferred_element_type=jnp.float32)
            precond = (gram / denominator).astype(jnp.bfloat16)
            mapped = jnp.dot(train_out, precond, preferred_element_type=jnp.float32)
            return jnp.sum(mapped * train_in.astype(jnp.float32), axis=1)

        values = lax.map(one_query, jnp.arange(QUERIES, dtype=jnp.int32))
        total = total + jnp.dot(values, train_onehot, precision=lax.Precision.HIGHEST)
    return total
```

```python
import jax
import jax.numpy as jnp
from jax import lax
from jax.sharding import PartitionSpec as P

QUERIES = 4
TRAIN = 16


def ring_pieces(blocks, col_count):
    up = [(s, (s + 1) % col_count) for s in range(col_count)]
    down = [(s, (s - 1) % col_count) for s in range(col_count)]
    steps = [blocks]
    for _ in range(col_count - 1):
        steps.append(
            [lax.ppermute(b, "col", down if i % 2 else up) for i, b in enumerate(steps[-1])]
        )
    return steps


def row_sum(term, row_count):
    if row_count == 2:
        other = lax.ppermute(term, "row", [(0, 1), (1, 0)])
        return (term.astype(jnp.float32) + other.astype(jnp.float32)).astype(jnp.bfloat16)
    return lax.psum(term, "row")


def body(
    activations,
    out_grads,
    basis_in,
    basis_out,
    eigenvalues,
    damping,
    layer_order,
    query_ids,
    train_ids,
):
    layer_groups = lax.axis_size("layer")
    row_count = lax.axis_size("row")
    col_count = lax.axis_size("col")
    me = lax.axis_index("col")
    query_tokens = query_ids.shape[0]

    ordered_in = jnp.take(activations, layer_order, axis=0)
    in_block = ordered_in.shape[1]
    moved_in = lax.all_to_all(ordered_in, "layer", split_axis=0, concat_axis=1, tiled=True)
    shaped_in = moved_in.reshape(layer_groups, in_block, moved_in.shape[2])
    joined_in = lax.all_gather(shaped_in, "row", axis=1, tiled=True)
    inputs_full = joined_in.reshape(layer_groups * row_count * in_block, moved_in.shape[2])
    partial_in = jnp.dot(inputs_full, basis_in[0], preferred_element_type=jnp.float32)
    rotated_in = lax.psum(partial_in.astype(jnp.bfloat16), "col")

    ordered_out = jnp.take(out_grads, layer_order, axis=0)
    block = ordered_out.shape[1]
    moved_out = lax.all_to_all(ordered_out, "layer", split_axis=0, concat_axis=1, tiled=True)
    moved_out = moved_out.reshape(layer_groups, block, moved_out.shape[2])

    def rotate(pieces):
        tokens = jnp.concatenate(pieces, axis=0)
        partial = jnp.dot(tokens, basis_out[0], preferred_element_type=jnp.float32)
        return row_sum(partial.astype(jnp.bfloat16), row_count)

    head = min(layer_groups, -(-query_tokens // (col_count * block)))
    first = ring_pieces([moved_out[l] for l in range(head)], col_count)
    second = ring_pieces([moved_out[l] for l in range(head, layer_groups)], col_count)

    def source(step, i):
        return lax.rem(me + (step if i % 2 else col_count - step), col_count)

    width = basis_out.shape[2]
    front = jnp.zeros((head, col_count, block, width), jnp.bfloat16)
    for begin in range(0, col_count, 2):
        steps = range(begin, min(begin + 2, col_count))
        rotated = rotate([b for s in steps for b in first[s]])
        rotated = rotated.reshape(len(steps), head, 1, block, width)
        for n, s in enumerate(steps):
            for i in range(head):
                front = lax.dynamic_update_slice(
                    front, rotated[n, i][None], (i, source(s, i), 0, 0)
                )
    front = front.reshape(head * col_count * block, width)

    query_mask = (query_ids[None, :] == jnp.arange(QUERIES, dtype=jnp.int32)[:, None]).astype(
        jnp.bfloat16
    )
    query_in = rotated_in[:query_tokens]
    query_out = front[:query_tokens]
    masked = query_mask[:, :, None] * query_in[None, :, :]
    query_gram = jnp.einsum("si,qsj->qij", query_out, masked, preferred_element_type=jnp.float32)
    precond = (query_gram / (eigenvalues[0] + damping[0])).astype(jnp.bfloat16)

    def scores_of(train_out, train_in, ids):
        onehot = (ids[:, None] == jnp.arange(TRAIN, dtype=jnp.int32)[None, :]).astype(jnp.float32)
        mapped = jnp.einsum("ui,qij->quj", train_out, precond, preferred_element_type=jnp.float32)
        values = jnp.sum(mapped * train_in[None, :, :], axis=2)
        return jnp.dot(values, onehot, precision=lax.Precision.HIGHEST)

    front_tokens = head * col_count * block
    total = jnp.zeros((QUERIES, TRAIN), jnp.float32)
    if front_tokens > query_tokens:
        total = total + scores_of(
            front[query_tokens:],
            rotated_in[query_tokens:front_tokens],
            train_ids[: front_tokens - query_tokens],
        )

    if head < layer_groups:
        groups = [list(range(b, min(b + 2, col_count))) for b in range(0, col_count, 2)]
        if len(groups[-1]) == 2:
            groups[-1:] = [[groups[-1][0]], [groups[-1][1]]]
        for steps in groups:
            train_out = rotate([b for s in steps for b in second[s]])
            train_in, ids = [], []
            for s in steps:
                for i in range(layer_groups - head):
                    start = ((head + i) * col_count + source(s, i)) * block
                    train_in.append(lax.dynamic_slice_in_dim(rotated_in, start, block, 0))
                    ids.append(lax.dynamic_slice_in_dim(train_ids, start - query_tokens, block, 0))
            total = total + scores_of(
                train_out, jnp.concatenate(train_in, axis=0), jnp.concatenate(ids, axis=0)
            )
    return lax.psum(total, ("layer", "col", "row"))


def solution(mesh):
    in_specs = (
        P(None, ("layer", "row"), "col"),
        P(None, ("layer", "col"), "row"),
        P("layer", "col", "row"),
        P("layer", "row", "col"),
        P("layer", "col", "row"),
        P("layer"),
        P(),
        P(),
        P(),
    )
    out_specs = P()
    return jax.shard_map(body, mesh=mesh, in_specs=in_specs, out_specs=out_specs, check_vma=False)
```
